128 devices in a mesh: row: 8 (over x, core), col: 16 (over y, z).
Axes of the slice: x: 4, y: 4, z: 4, core: 2. Of those that a mesh axis runs over, the one named last changes fastest.
Arguments:
- tiles: bfloat16 [8, 16, 128, 128, 128], P('row', 'col')
- tile_row: int32 [8, 16, 128], P('row', 'col'), may hold values from 0 to 15, as said below
- tile_col: int32 [8, 16, 128], P('row', 'col'), may hold values from 0 to 15
- tile_count: int32 [8, 16], P('row', 'col'), may hold values from 1 to 128, as said below
- sinogram: float32 [8, 2048, 128], P('row', 'col')
Outputs:
- volume: float32 [16, 2048, 128], P('col', 'row')
- residual: float32 [8, 2048, 128], P('row', 'col')
The draws below stay inside these ranges and needn't reach their ends.
Inputs may be any that keep to these rules, and one draw needn't show every extreme that they name: Within one block the pairs (tile_row, tile_col) of all 128 slots are distinct. Slots 0 to tile_count - 1 of a block are live, the rest are ignored; some block has all 128 slots live in every draw.
All inputs are finite; a program needn't handle non-finite values.
Results may differ from the reference program's by a relative error of at most 0.015.
Values may be sent and summed in bfloat16 or wider, within the bound.
A program may use at most 64 MiB of HBM per device.

```python
import jax
import jax.numpy as jnp
from jax import lax

TILE = 128
RT = 16
VT = 16
TMAX = 128
FRAMES = 128
ITERS = 4
RAYS = 2048
VOX = 2048
N_ROW = 8
N_COL = 16


def tile_pairs(key):
    keys = jax.random.split(jax.random.fold_in(key, 7), N_ROW * N_COL)

    def shuffled(single):
        return jax.random.permutation(single, jnp.arange(RT * VT, dtype=jnp.int32))
    order = jax.vmap(shuffled)(keys)[:, :TMAX]
    rows = (order // VT).reshape(N_ROW, N_COL, TMAX).astype(jnp.int32)
    cols = (order % VT).reshape(N_ROW, N_COL, TMAX).astype(jnp.int32)
    return (rows, cols)


def draw_tile_row(key, part):
    return tile_pairs(key)[0]


def draw_tile_col(key, part):
    return tile_pairs(key)[1]


def draw_tile_count(key, part):
    base = TMAX // 8 + jax.random.randint(jax.random.fold_in(key, 3), (N_ROW * N_COL,), 0, TMAX // 2 + 1)
    base = jnp.maximum(base, 1)
    fullest = jax.random.randint(jax.random.fold_in(key, 5), (), 0, N_ROW * N_COL)
    base = jnp.where(jnp.arange(N_ROW * N_COL, dtype=jnp.int32) == fullest, TMAX, base)
    return base.reshape(N_ROW, N_COL).astype(jnp.int32)


def draw_tiles(key, part):
    shape = (N_ROW, N_COL, TMAX, TILE, TILE)
    place = lax_index(shape)
    rising = 3.0 ** (place / max(N_ROW * N_COL - 1, 1))
    fan = (TILE * N_COL * TMAX // (2 * RT)) ** (-0.5)
    values = jax.random.normal(jax.random.fold_in(key, 11), shape, jnp.float32)
    return (values * rising * fan).astype(jnp.bfloat16)


def lax_index(shape):
    first = jax.lax.broadcasted_iota(jnp.float32, shape, 0)
    second = jax.lax.broadcasted_iota(jnp.float32, shape, 1)
    return first * N_COL + second


def draw_sinogram(key, part):
    shape = (N_ROW, RAYS, FRAMES)
    ray = jax.lax.broadcasted_iota(jnp.float32, shape, 0) * RAYS + jax.lax.broadcasted_iota(jnp.float32, shape, 1)
    rising = 3.0 ** (ray / (N_ROW * RAYS - 1))
    values = jnp.clip(jax.random.normal(jax.random.fold_in(key, 17), shape, jnp.float32), -6.0, 6.0)
    return values * rising * 0.25


def setup_inputs(seed: int = 0) -> dict:
    key_of = jax.random.split(jax.random.key(seed), 6)
    return {
        "tiles": draw_tiles(jax.random.fold_in(key_of[5], 71), 0),
        "tile_row": draw_tile_row(jax.random.fold_in(key_of[5], 71), 0),
        "tile_col": draw_tile_col(jax.random.fold_in(key_of[5], 71), 0),
        "tile_count": draw_tile_count(jax.random.fold_in(key_of[5], 71), 0),
        "sinogram": draw_sinogram(jax.random.fold_in(key_of[5], 71), 0),
    }


def tile_pick(table, index):
    return lax.optimization_barrier(jnp.take(table, index, axis=0))


def forward_block(blocks, rows_index, cols_index, count, voxel_tiles):
    picked = tile_pick(voxel_tiles, cols_index)
    products = jnp.einsum("tij,tjk->tik", blocks.astype(jnp.float32), picked.astype(jnp.float32))
    live = jnp.arange(TMAX, dtype=jnp.int32) < count
    select = ((rows_index[None, :] == jnp.arange(RT, dtype=jnp.int32)[:, None]) & live[None, :]).astype(jnp.float32)
    return jnp.einsum("ut,tik->uik", select, products, precision=lax.Precision.HIGHEST)


def backward_block(blocks, rows_index, cols_index, count, ray_tiles):
    picked = tile_pick(ray_tiles, rows_index)
    products = jnp.einsum("tji,tjk->tik", blocks.astype(jnp.float32), picked.astype(jnp.float32))
    live = jnp.arange(TMAX, dtype=jnp.int32) < count
    select = ((cols_index[None, :] == jnp.arange(VT, dtype=jnp.int32)[:, None]) & live[None, :]).astype(jnp.float32)
    return jnp.einsum("ut,tik->uik", select, products, precision=lax.Precision.HIGHEST)


def reference(tiles, tile_row, tile_col, tile_count, sinogram):
    blocks_all = tiles.reshape(N_ROW * N_COL, TMAX, TILE, TILE)
    rows_all = tile_row.reshape(N_ROW * N_COL, TMAX)
    cols_all = tile_col.reshape(N_ROW * N_COL, TMAX)
    counts_all = tile_count.reshape(N_ROW * N_COL)
    devices = jnp.arange(N_ROW * N_COL, dtype=jnp.int32)

    def apply_forward(direction):
        voxel_tiles = direction.astype(jnp.bfloat16).reshape(N_COL, VT, TILE, FRAMES)

        def single(device):
            return forward_block(blocks_all[device], rows_all[device], cols_all[device],
                                 counts_all[device], voxel_tiles[device % N_COL])

        parts = lax.map(single, devices)
        return parts.reshape(N_ROW, N_COL, RAYS, FRAMES).sum(axis=1)

    def apply_backward(field):
        ray_tiles = field.astype(jnp.bfloat16).reshape(N_ROW, RT, TILE, FRAMES)

        def single(device):
            return backward_block(blocks_all[device], rows_all[device], cols_all[device],
                                  counts_all[device], ray_tiles[device // N_COL])

        parts = lax.map(single, devices)
        return parts.reshape(N_ROW, N_COL, VOX, FRAMES).sum(axis=0)

    volume = jnp.zeros((N_COL, VOX, FRAMES), jnp.float32)
    residual = sinogram
    search = apply_backward(residual)
    gamma = jnp.sum(search * search, axis=(0, 1))
    direction = search
    for step in range(ITERS):
        image = apply_forward(direction)
        alpha = gamma / jnp.sum(image * image, axis=(0, 1))
        volume = volume + alpha * direction
        residual = residual - alpha * image
        if step + 1 < ITERS:
            search = apply_backward(residual)
            fresh = jnp.sum(search * search, axis=(0, 1))
            direction = search + (fresh / gamma) * direction
            gamma = fresh
    return volume, residual
```

```python
import functools

import jax
import jax.numpy as jnp
from jax import lax
from jax.experimental import pallas as pl
from jax.experimental.pallas import tpu as pltpu
from jax.sharding import PartitionSpec as P

TILE = 128
NT = 16
ITERS = 4
NX = 4
N_ROW = 8
N_COL = 16
FRAMES = 128
RAYS = NT * TILE
VOX = NT * TILE
VP = VOX // N_ROW
RP = RAYS // N_COL
GROUPS = 2
M = FRAMES // GROUPS
MESH = pl.DeviceIdType.MESH
F32 = jnp.float32
BF16 = jnp.bfloat16

COL_PAIRS = (
    ((2, 2), (2, 1)),
    ((2, 3), (1, 2)),
    ((3, 2), (2, 0)),
    ((0, 2), (1, 1)),
    ((1, 3), (3, 1)),
    ((3, 3), (1, 0)),
    ((3, 0), (0, 1)),
    ((0, 3), (0, 0)),
)
COL_PEERS = tuple(d for pair in COL_PAIRS for d in pair)[:-1]
ROW_PEERS = tuple((dx, dc) for dx in (2, 1, 3, 0) for dc in (1, 0))[:-1]
X_PEERS = (2, 1, 3)
BATCHES = (2, 3, 3)
FIRST = 0.6


def frame_squares(x):
    total = None
    for i in range(x.shape[1] // 128):
        part = x[:, i * 128 : (i + 1) * 128].astype(F32)
        total = part * part if total is None else total + part * part
    if M < 128:
        total = jnp.concatenate([total, jnp.zeros((128 - M, 128), F32)], axis=0)
    return jnp.sum(total.T, axis=0, keepdims=True)


def per_frame(*rows):
    stack = jnp.concatenate([*rows, jnp.zeros((8 - len(rows), 128), F32)], axis=0).T
    return [stack[:M, i : i + 1] for i in range(len(rows))]


def kernel(
    slot_of, tiles, sino, vol_out, res_out,
    tl, tlt, a, at, u, v, dsend, drecv, rsend, rrecv, csend, crecv, own_r, own_c,
    s, d, im, vol, res, gam, step, guess, nr_send, nr_recv, ng_send, ng_recv, ni_send, ni_recv,
    tsem, u_ss, u_rs, v_ss, v_rs, f_ss, d_ss, d_rs, r_ss, r_rs, c_ss, c_rs, nr_ss, nr_rs, ng_ss, ng_rs, ni_ss, ni_rs,
):
    row = lax.axis_index("row")
    col = lax.axis_index("col")
    x, core = row // 2, row % 2
    y, z = col // 4, col % 4

    def row_of(dx, dc):
        return ((x + dx) % 4) * 2 + (core + dc) % 2

    def col_of(dy, dz):
        return ((y + dy) % 4) * 4 + (z + dz) % 4

    def remote(src, dst, ss, rs, to_row, to_col):
        return pltpu.make_async_remote_copy(
            src_ref=src, dst_ref=dst, send_sem=ss, recv_sem=rs, device_id=(to_row, to_col), device_id_type=MESH
        )

    def arrived(ref, sem):
        remote(ref, ref, sem, sem, row, col).wait_recv()

    def sent(ref, sem):
        remote(ref, ref, sem, sem, row, col).wait_send()

    n_col, n_row = len(COL_PEERS), len(ROW_PEERS)

    def send_field(g):
        for dy, dz in COL_PEERS:
            remote(u.at[g, col], u.at[g, col], u_ss.at[g], u_rs.at[g], row, col_of(dy, dz)).start()

    def send_norm(g, i_send, i_recv, ss, rs):
        for i, (dy, dz) in enumerate(COL_PEERS):
            remote(i_send.at[g], i_recv.at[g, i], ss.at[g], rs.at[g], row, col_of(dy, dz)).start()

    def send_row_norm(g):
        for i, (dx, dc) in enumerate(ROW_PEERS):
            remote(nr_send.at[g], nr_recv.at[g, i], nr_ss.at[g], nr_rs.at[g], row_of(dx, dc), col).start()

    def half(i):
        return pl.ds(2 * i, 2)

    def d_send(g, i):
        return remote(dsend.at[g, half(i)], drecv.at[g, half(i)], d_ss.at[g, i], d_rs.at[g, i], row_of(0, 1), col)

    def r_send(g, i):
        return remote(rsend.at[g, i], rrecv.at[g, i], r_ss.at[g], r_rs.at[g], row_of(X_PEERS[i], 0), col)

    def c_send(g, i):
        return remote(csend.at[g, i], crecv.at[g, i], c_ss.at[g], c_rs.at[g], row, col_of(*COL_PEERS[i]))

    def v_send(g, i):
        to = row_of(X_PEERS[i], 0) if i < 3 else row_of(0, 1)
        return remote(v.at[g, row], v.at[g, row], v_ss.at[g], v_rs.at[g, i], to, col)

    def f_send(g, i):
        slot = v.at[g, row_of(-X_PEERS[i], 0)]
        return remote(slot, slot, f_ss.at[g], v_rs.at[g, 3], row_of(0, 1), col)

    def voxel_product(field, n):
        block = a[:, pl.ds(pl.multiple_of(n * VP, VP), VP)]
        return jnp.dot(field, block, preferred_element_type=F32)

    def ray_product(field, first, second):
        columns = [at[:, pl.ds(pl.multiple_of(c * RP, RP), RP)] for c in (first, second)]
        return jnp.dot(field, jnp.concatenate(columns, axis=1), preferred_element_type=F32)

    def pass_norm(g):
        arrived(ni_recv.at[g, pl.ds(0, n_col)], ni_rs.at[g])
        squares = jnp.sum(ni_recv[g].reshape(N_COL, 128), axis=0, keepdims=True)
        nr_send[g] = squares
        nr_recv[g, n_row] = squares
        send_row_norm(g)
        sent(ni_recv.at[g, pl.ds(0, n_col)], ni_ss.at[g])

    def total_norm(g):
        arrived(nr_recv.at[g, pl.ds(0, n_row)], nr_rs.at[g])
        sent(nr_recv.at[g, pl.ds(0, n_row)], nr_ss.at[g])
        return jnp.sum(nr_recv[g].reshape(N_ROW, 128), axis=0, keepdims=True)

    def back_project(g):
        arrived(u.at[g, pl.ds(0, n_col)], u_rs.at[g])
        field = jnp.concatenate([u[g, i] for i in range(N_COL)], axis=1)
        order = (*X_PEERS, 0)
        for h in range(2):
            for i in (2 * h, 2 * h + 1):
                dsend[g, i] = voxel_product(field, row_of(order[i], 1)).astype(BF16)
            d_send(g, h).start()
        for i in range(4):
            own_r[g, i] = voxel_product(field, row_of(order[i], 0))
        pass_norm(g)
        for h in range(2):
            d_send(g, h).wait_recv()
            for i in (2 * h, 2 * h + 1):
                part = own_r[g, i] + drecv[g, i].astype(F32)
                if i < 3:
                    rsend[g, i] = part.astype(BF16)
                    r_send(g, i).start()
                else:
                    own_r[g, i] = part
        sent(u.at[g, pl.ds(0, n_col)], u_ss.at[g])

    def new_search(g, k):
        norm = total_norm(g)
        new_step = jnp.where(k == 0, FIRST * norm, gam[g] / norm)
        alpha, share = per_frame(new_step, jnp.where(k == 0, 1.0, new_step / guess[g]))
        step[g] = new_step
        arrived(rrecv.at[g], r_rs.at[g])
        total = own_r[g, 3]
        for i in range(3):
            total = total + rrecv[g, i].astype(F32)
        fresh = share * total + (1.0 - share) * s[g]
        s[g] = fresh
        v[g, row] = fresh.astype(BF16)
        for i in range(4):
            v_send(g, i).start()
        vol[g] = vol[g] + alpha * d[g]
        res[g] = res[g] - alpha * im[g]
        for h in range(2):
            d_send(g, h).wait_send()
        sent(rsend.at[g], r_ss.at[g])

    def project(g):
        for i in (1, 2, 0):
            slot = v.at[g, row_of(-X_PEERS[i], 0)]
            arrived(slot, v_rs.at[g, i])
            f_send(g, i).start()
        arrived(v.at[g, pl.ds(0, 4)], v_rs.at[g, 3])
        field = jnp.concatenate([v[g, i] for i in range(N_ROW)], axis=1)
        done = 0
        for many in BATCHES:
            for p in range(done, done + many):
                first, second = COL_PAIRS[p]
                part = ray_product(field, col_of(*first), col_of(*second))
                csend[g, 2 * p] = part[:, :RP].astype(BF16)
                if 2 * p + 1 < n_col:
                    csend[g, 2 * p + 1] = part[:, RP:].astype(BF16)
                else:
                    own_c[g] = part[:, RP:]
            if done == 0:
                squares = frame_squares(field)
                ng_send[g] = squares
                ng_recv[g, n_col] = squares
            for i in range(2 * done, min(2 * (done + many), n_col)):
                c_send(g, i).start()
            if done == 0:
                send_norm(g, ng_send, ng_recv, ng_ss, ng_rs)
            done += many
        sent(v.at[g, pl.ds(0, 4)], v_ss.at[g])
        sent(v.at[g, pl.ds(0, 3)], f_ss.at[g])

    def new_image(g, k):
        arrived(ng_recv.at[g, pl.ds(0, n_col)], ng_rs.at[g])
        gamma = jnp.sum(ng_recv[g].reshape(N_COL, 128), axis=0, keepdims=True)
        ahead = jnp.where(k == 0, step[g] / gamma, step[g])
        ahead = jnp.where((ahead > 1e-30) & (ahead < 1e30), ahead, 1.0)
        beta, trial = per_frame(jnp.where(k == 0, 0.0, gamma / gam[g]), ahead)
        gam[g] = gamma
        guess[g] = ahead
        arrived(crecv.at[g], c_rs.at[g])
        total = own_c[g]
        for i in range(n_col):
            total = total + crecv[g, i].astype(F32)
        image = total + beta * im[g]
        im[g] = image

        @pl.when(k + 1 < ITERS)
        def _():
            u[g, col] = (res[g] - trial * image).astype(BF16)
            send_field(g)

        squares = frame_squares(image)
        ni_send[g] = squares
        ni_recv[g, n_col] = squares
        send_norm(g, ni_send, ni_recv, ni_ss, ni_rs)
        d[g] = s[g] + beta * d[g]
        sent(csend.at[g], c_ss.at[g])
        sent(ng_recv.at[g, pl.ds(0, n_col)], ng_ss.at[g])

    load = pltpu.make_async_copy(tiles, tl.at[pl.ds(0, TILE)], tsem)
    load.start()
    barrier = pltpu.get_barrier_semaphore()
    for dy, dz in COL_PEERS:
        pl.semaphore_signal(barrier, inc=1, device_id=(row, col_of(dy, dz)), device_id_type=MESH)
    for dx, dc in ROW_PEERS:
        pl.semaphore_signal(barrier, inc=1, device_id=(row_of(dx, dc), col), device_id_type=MESH)
    first = sino[...].T
    for g in range(GROUPS):
        measured = first[g * M : (g + 1) * M]
        res[g] = measured
        u[g, col] = measured.astype(BF16)
        squares = frame_squares(measured)
        ni_send[g] = squares
        ni_recv[g, n_col] = squares
        s[g] = jnp.zeros((M, VP), F32)
        d[g] = jnp.zeros((M, VP), F32)
        vol[g] = jnp.zeros((M, VP), F32)
        im[g] = jnp.zeros((M, RP), F32)
        gam[g] = jnp.ones((1, 128), F32)
        guess[g] = jnp.ones((1, 128), F32)
    tl[TILE] = jnp.zeros((TILE, TILE), BF16)
    pl.semaphore_wait(barrier, n_col + n_row)
    for g in range(GROUPS):
        send_field(g)
        send_norm(g, ni_send, ni_recv, ni_ss, ni_rs)
    load.wait()

    def place(i, carry):
        for j in range(NT):
            rows = pl.ds(pl.multiple_of(i * TILE, TILE), TILE)
            a[rows, j * TILE : (j + 1) * TILE] = tl[slot_of[i * NT + j]]
        return carry

    lax.fori_loop(0, NT, place, 0)

    def turn():
        def one(t, carry):
            for i in range(8):
                tlt[t * 8 + i] = tl[t * 8 + i].T
            return carry

        lax.fori_loop(0, TILE // 8, one, 0)
        tlt[TILE] = jnp.zeros((TILE, TILE), BF16)

        def place_turned(i, carry):
            for j in range(NT):
                columns = pl.ds(pl.multiple_of(i * TILE, TILE), TILE)
                at[j * TILE : (j + 1) * TILE, columns] = tlt[slot_of[i * NT + j]]
            return carry

        lax.fori_loop(0, NT, place_turned, 0)

    def iteration(k, carry):
        back_project(0)

        @pl.when(k == 0)
        def _():
            turn()

        if GROUPS == 1:
            new_search(0, k)
            project(0)
            new_image(0, k)
            return carry

        @pl.when(k > 0)
        def _():
            new_image(1, k - 1)

        new_search(0, k)
        back_project(1)
        project(0)
        new_search(1, k)
        new_image(0, k)
        project(1)
        return carry

    lax.fori_loop(0, ITERS, iteration, 0)

    def finish(g):
        (alpha,) = per_frame(gam[g] / total_norm(g))
        return vol[g] + alpha * d[g], res[g] - alpha * im[g]

    if GROUPS == 2:
        new_image(1, ITERS - 1)
    done = []
    for g in range(GROUPS):
        pass_norm(g)
    for g in range(GROUPS):
        done.append(finish(g))
    vol_out[...] = jnp.concatenate([volume for volume, _ in done], axis=0).T
    res_out[...] = jnp.concatenate([residual for _, residual in done], axis=0).T


def local(tiles, tile_row, tile_col, tile_count, sinogram):
    live = jnp.arange(TILE, dtype=jnp.int32) < tile_count[0, 0]
    place = jnp.where(live, tile_row[0, 0] * NT + tile_col[0, 0], -1)
    slots = jnp.arange(TILE, dtype=jnp.int32)
    here = place[None, :] == jnp.arange(NT * NT, dtype=jnp.int32)[:, None]
    slot_of = jnp.min(jnp.where(here, slots[None, :], TILE), axis=1)
    dma = pltpu.SemaphoreType.DMA
    vm = pltpu.VMEM
    G, nc = GROUPS, len(COL_PEERS)
    volume, residual = pl.pallas_call(
        kernel,
        out_shape=(jax.ShapeDtypeStruct((VP, FRAMES), F32), jax.ShapeDtypeStruct((RP, FRAMES), F32)),
        in_specs=[
            pl.BlockSpec(memory_space=pltpu.SMEM),
            pl.BlockSpec(memory_space=pl.ANY),
            pl.BlockSpec(memory_space=pltpu.VMEM),
        ],
        out_specs=(pl.BlockSpec(memory_space=pltpu.VMEM), pl.BlockSpec(memory_space=pltpu.VMEM)),
        scratch_shapes=[
            vm((TILE + 1, TILE, TILE), BF16), vm((TILE + 1, TILE, TILE), BF16),
            vm((RAYS, VOX), BF16), vm((VOX, RAYS), BF16),
            vm((G, N_COL, M, RP), BF16), vm((G, N_ROW, M, VP), BF16),
            vm((G, 4, M, VP), BF16), vm((G, 4, M, VP), BF16), vm((G, 3, M, VP), BF16), vm((G, 3, M, VP), BF16),
            vm((G, nc, M, RP), BF16), vm((G, nc, M, RP), BF16),
            vm((G, 4, M, VP), F32), vm((G, M, RP), F32),
            vm((G, M, VP), F32), vm((G, M, VP), F32), vm((G, M, RP), F32), vm((G, M, VP), F32), vm((G, M, RP), F32),
            vm((G, 1, 128), F32), vm((G, 1, 128), F32), vm((G, 1, 128), F32),
            vm((G, 1, 128), F32), vm((G, N_ROW, 1, 128), F32),
            vm((G, 1, 128), F32), vm((G, N_COL, 1, 128), F32), vm((G, 1, 128), F32), vm((G, N_COL, 1, 128), F32),
            dma, dma((G,)), dma((G,)), dma((G,)), dma((G, 4)), dma((G,)), dma((G, 2)), dma((G, 2)), dma((G,)), dma((G,)),
            dma((G,)), dma((G,)), dma((G,)), dma((G,)), dma((G,)), dma((G,)), dma((G,)), dma((G,)),
        ],
        compiler_params=pltpu.CompilerParams(
            collective_id=0, has_side_effects=True, vmem_limit_bytes=60 * 1024 * 1024
        ),
    )(slot_of, tiles[0, 0], sinogram[0])
    return (volume[None], residual[None])


def solution(mesh):
    placed = (
        P("row", "col", None, None, None),
        P("row", "col", None),
        P("row", "col", None),
        P("row", "col"),
        P("row", "col", None),
    )
    return jax.shard_map(
        local,
        mesh=mesh,
        in_specs=placed,
        out_specs=(P("col", "row", None), P("row", "col", None)),
        check_vma=False,
    )
```

```python
import functools

import jax
import jax.numpy as jnp
from jax import lax
from jax.experimental import pallas as pl
from jax.experimental.pallas import tpu as pltpu
from jax.sharding import PartitionSpec as P

TILE = 128
NT = 16
ITERS = 4
NX = 4
N_ROW = 8
N_COL = 16
FRAMES = 128
RAYS = NT * TILE
VOX = NT * TILE
VP = VOX // N_ROW
RP = RAYS // N_COL
GROUPS = 2
M = FRAMES // GROUPS
MESH = pl.DeviceIdType.MESH
F32 = jnp.float32
BF16 = jnp.bfloat16

COL_PAIRS = (
    ((2, 2), (2, 1)),
    ((2, 3), (1, 2)),
    ((3, 2), (2, 0)),
    ((0, 2), (1, 1)),
    ((1, 3), (3, 1)),
    ((3, 3), (1, 0)),
    ((3, 0), (0, 1)),
    ((0, 3), (0, 0)),
)
COL_PEERS = tuple(d for pair in COL_PAIRS for d in pair)[:-1]
ROW_PEERS = tuple((dx, dc) for dx in (2, 1, 3, 0) for dc in (1, 0))[:-1]
BACK_BATCHES = (2, 3, 3)
BATCHES = (2, 3, 3)
FIRST = 0.6


def frame_squares(x):
    total = None
    for i in range(x.shape[1] // 128):
        part = x[:, i * 128 : (i + 1) * 128].astype(F32)
        total = part * part if total is None else total + part * part
    if M < 128:
        total = jnp.concatenate([total, jnp.zeros((128 - M, 128), F32)], axis=0)
    return jnp.sum(total.T, axis=0, keepdims=True)


def per_frame(*rows):
    stack = jnp.concatenate([*rows, jnp.zeros((8 - len(rows), 128), F32)], axis=0).T
    return [stack[:M, i : i + 1] for i in range(len(rows))]


def kernel(
    slot_of, tiles, sino, vol_out, res_out,
    tl, a, at, u, v, rsend, rrecv, csend, crecv, own_r, own_c,
    s, d, im, vol, res, gam, step, guess, nr_send, nr_recv, ng_send, ng_recv, ni_send, ni_recv,
    tsem, u_ss, u_rs, v_ss, v_rs, r_ss, r_rs, c_ss, c_rs, nr_ss, nr_rs, ng_ss, ng_rs, ni_ss, ni_rs,
):
    row = lax.axis_index("row")
    col = lax.axis_index("col")
    x, core = row // 2, row % 2
    y, z = col // 4, col % 4

    def row_of(dx, dc):
        return ((x + dx) % 4) * 2 + (core + dc) % 2

    def col_of(dy, dz):
        return ((y + dy) % 4) * 4 + (z + dz) % 4

    def remote(src, dst, ss, rs, to_row, to_col):
        return pltpu.make_async_remote_copy(
            src_ref=src, dst_ref=dst, send_sem=ss, recv_sem=rs, device_id=(to_row, to_col), device_id_type=MESH
        )

    def arrived(ref, sem):
        remote(ref, ref, sem, sem, row, col).wait_recv()

    def sent(ref, sem):
        remote(ref, ref, sem, sem, row, col).wait_send()

    n_col, n_row = len(COL_PEERS), len(ROW_PEERS)

    def send_field(g):
        for dy, dz in COL_PEERS:
            remote(u.at[g, col], u.at[g, col], u_ss.at[g], u_rs.at[g], row, col_of(dy, dz)).start()

    def send_norm(g, i_send, i_recv, ss, rs):
        for i, (dy, dz) in enumerate(COL_PEERS):
            remote(i_send.at[g], i_recv.at[g, i], ss.at[g], rs.at[g], row, col_of(dy, dz)).start()

    def send_row_norm(g):
        for i, (dx, dc) in enumerate(ROW_PEERS):
            remote(nr_send.at[g], nr_recv.at[g, i], nr_ss.at[g], nr_rs.at[g], row_of(dx, dc), col).start()

    def r_send(g, i):
        return remote(rsend.at[g, i], rrecv.at[g, i], r_ss.at[g], r_rs.at[g], row_of(*ROW_PEERS[i]), col)

    def c_send(g, i):
        return remote(csend.at[g, i], crecv.at[g, i], c_ss.at[g], c_rs.at[g], row, col_of(*COL_PEERS[i]))

    def send_search(g):
        for dx, dc in ROW_PEERS:
            remote(v.at[g, row], v.at[g, row], v_ss.at[g], v_rs.at[g], row_of(dx, dc), col).start()

    def voxel_product(field, n):
        block = jnp.concatenate([a[2 * n], a[2 * n + 1]], axis=1)
        return jnp.dot(field, block, preferred_element_type=F32)

    def ray_product(field, first, second):
        block = jnp.concatenate([at[first], at[second]], axis=1)
        return jnp.dot(field, block, preferred_element_type=F32)

    def pass_norm(g):
        arrived(ni_recv.at[g, pl.ds(0, n_col)], ni_rs.at[g])
        squares = jnp.sum(ni_recv[g].reshape(N_COL, 128), axis=0, keepdims=True)
        nr_send[g] = squares
        nr_recv[g, n_row] = squares
        send_row_norm(g)
        sent(ni_recv.at[g, pl.ds(0, n_col)], ni_ss.at[g])

    def total_norm(g):
        arrived(nr_recv.at[g, pl.ds(0, n_row)], nr_rs.at[g])
        sent(nr_recv.at[g, pl.ds(0, n_row)], nr_ss.at[g])
        return jnp.sum(nr_recv[g].reshape(N_ROW, 128), axis=0, keepdims=True)

    def back_project(g):
        arrived(u.at[g, pl.ds(0, n_col)], u_rs.at[g])
        field = jnp.concatenate([u[g, i] for i in range(N_COL)], axis=1)
        done = 0
        for many in BACK_BATCHES:
            for i in range(done, done + many):
                if i < n_row:
                    rsend[g, i] = voxel_product(field, row_of(*ROW_PEERS[i])).astype(BF16)
                else:
                    own_r[g] = voxel_product(field, row)
            for i in range(done, min(done + many, n_row)):
                r_send(g, i).start()
            if done == 0:
                pass_norm(g)
            done += many
        sent(u.at[g, pl.ds(0, n_col)], u_ss.at[g])

    def new_search(g, k):
        norm = total_norm(g)
        new_step = jnp.where(k == 0, FIRST * norm, gam[g] / norm)
        alpha, share = per_frame(new_step, jnp.where(k == 0, 1.0, new_step / guess[g]))
        step[g] = new_step
        arrived(rrecv.at[g], r_rs.at[g])
        total = own_r[g]
        for i in range(n_row):
            total = total + rrecv[g, i].astype(F32)
        fresh = share * total + (1.0 - share) * s[g]
        s[g] = fresh
        v[g, row] = fresh.astype(BF16)
        send_search(g)
        vol[g] = vol[g] + alpha * d[g]
        res[g] = res[g] - alpha * im[g]
        sent(rsend.at[g], r_ss.at[g])

    def project(g):
        arrived(v.at[g, pl.ds(0, n_row)], v_rs.at[g])
        field = jnp.concatenate([v[g, i] for i in range(N_ROW)], axis=1)
        done = 0
        for many in BATCHES:
            for p in range(done, done + many):
                first, second = COL_PAIRS[p]
                part = ray_product(field, col_of(*first), col_of(*second))
                csend[g, 2 * p] = part[:, :RP].astype(BF16)
                if 2 * p + 1 < n_col:
                    csend[g, 2 * p + 1] = part[:, RP:].astype(BF16)
                else:
                    own_c[g] = part[:, RP:]
            if done == 0:
                squares = frame_squares(field)
                ng_send[g] = squares
                ng_recv[g, n_col] = squares
            for i in range(2 * done, min(2 * (done + many), n_col)):
                c_send(g, i).start()
            if done == 0:
                send_norm(g, ng_send, ng_recv, ng_ss, ng_rs)
            done += many
        sent(v.at[g, pl.ds(0, n_row)], v_ss.at[g])

    def new_image(g, k):
        arrived(ng_recv.at[g, pl.ds(0, n_col)], ng_rs.at[g])
        gamma = jnp.sum(ng_recv[g].reshape(N_COL, 128), axis=0, keepdims=True)
        ahead = jnp.where(k == 0, step[g] / gamma, step[g])
        ahead = jnp.where((ahead > 1e-30) & (ahead < 1e30), ahead, 1.0)
        beta, trial = per_frame(jnp.where(k == 0, 0.0, gamma / gam[g]), ahead)
        gam[g] = gamma
        guess[g] = ahead
        arrived(crecv.at[g], c_rs.at[g])
        total = own_c[g]
        for i in range(n_col):
            total = total + crecv[g, i].astype(F32)
        image = total + beta * im[g]
        im[g] = image

        @pl.when(k + 1 < ITERS)
        def _():
            u[g, col] = (res[g] - trial * image).astype(BF16)
            send_field(g)

        squares = frame_squares(image)
        ni_send[g] = squares
        ni_recv[g, n_col] = squares
        send_norm(g, ni_send, ni_recv, ni_ss, ni_rs)
        d[g] = s[g] + beta * d[g]
        sent(csend.at[g], c_ss.at[g])
        sent(ng_recv.at[g, pl.ds(0, n_col)], ng_ss.at[g])

    load = pltpu.make_async_copy(tiles, tl.at[pl.ds(0, TILE)], tsem)
    load.start()
    barrier = pltpu.get_barrier_semaphore()
    for dy, dz in COL_PEERS:
        pl.semaphore_signal(barrier, inc=1, device_id=(row, col_of(dy, dz)), device_id_type=MESH)
    for dx, dc in ROW_PEERS:
        pl.semaphore_signal(barrier, inc=1, device_id=(row_of(dx, dc), col), device_id_type=MESH)
    first = sino[...].T
    for g in range(GROUPS):
        measured = first[g * M : (g + 1) * M]
        res[g] = measured
        u[g, col] = measured.astype(BF16)
        squares = frame_squares(measured)
        ni_send[g] = squares
        ni_recv[g, n_col] = squares
        s[g] = jnp.zeros((M, VP), F32)
        d[g] = jnp.zeros((M, VP), F32)
        vol[g] = jnp.zeros((M, VP), F32)
        im[g] = jnp.zeros((M, RP), F32)
        gam[g] = jnp.ones((1, 128), F32)
        guess[g] = jnp.ones((1, 128), F32)
    tl[TILE] = jnp.zeros((TILE, TILE), BF16)
    pl.semaphore_wait(barrier, n_col + n_row)
    for g in range(GROUPS):
        send_field(g)
        send_norm(g, ni_send, ni_recv, ni_ss, ni_rs)
    load.wait()

    def place(i, carry):
        for j in range(NT):
            rows = pl.ds(pl.multiple_of(i * TILE, TILE), TILE)
            a[j, rows, :] = tl[slot_of[i * NT + j]]
        return carry

    lax.fori_loop(0, NT, place, 0)

    def turn():
        places = [lax.broadcasted_iota(jnp.int32, (2 * TILE, 2 * TILE), i) for i in range(2)]
        one = jnp.where(places[0] == places[1], 1.0, 0.0).astype(BF16)

        def rows(i, carry):
            here = pl.ds(pl.multiple_of(i * 2 * TILE, 2 * TILE), 2 * TILE)
            for j in range(NT // 2):
                block = jnp.concatenate([a[2 * j, here, :], a[2 * j + 1, here, :]], axis=1)
                turned = lax.dot_general(one, block, (((1,), (1,)), ((), ())), preferred_element_type=F32).astype(BF16)
                at[2 * i, j * 2 * TILE : (j + 1) * 2 * TILE, :] = turned[:, :TILE]
                at[2 * i + 1, j * 2 * TILE : (j + 1) * 2 * TILE, :] = turned[:, TILE:]
            return carry

        lax.fori_loop(0, NT // 2, rows, 0)

    def iteration(k, carry):
        back_project(0)

        @pl.when(k == 0)
        def _():
            turn()

        if GROUPS == 1:
            new_search(0, k)
            project(0)
            new_image(0, k)
            return carry

        @pl.when(k > 0)
        def _():
            new_image(1, k - 1)

        new_search(0, k)
        back_project(1)
        project(0)
        new_search(1, k)
        new_image(0, k)
        project(1)
        return carry

    lax.fori_loop(0, ITERS, iteration, 0)

    def finish(g):
        (alpha,) = per_frame(gam[g] / total_norm(g))
        return vol[g] + alpha * d[g], res[g] - alpha * im[g]

    if GROUPS == 2:
        new_image(1, ITERS - 1)
    done = []
    for g in range(GROUPS):
        pass_norm(g)
    for g in range(GROUPS):
        done.append(finish(g))
    vol_out[...] = jnp.concatenate([volume for volume, _ in done], axis=0).T
    res_out[...] = jnp.concatenate([residual for _, residual in done], axis=0).T


def local(tiles, tile_row, tile_col, tile_count, sinogram):
    live = jnp.arange(TILE, dtype=jnp.int32) < tile_count[0, 0]
    place = jnp.where(live, tile_row[0, 0] * NT + tile_col[0, 0], -1)
    slots = jnp.arange(TILE, dtype=jnp.int32)
    here = place[None, :] == jnp.arange(NT * NT, dtype=jnp.int32)[:, None]
    slot_of = jnp.min(jnp.where(here, slots[None, :], TILE), axis=1)
    dma = pltpu.SemaphoreType.DMA
    vm = pltpu.VMEM
    G, nc, nr = GROUPS, len(COL_PEERS), len(ROW_PEERS)
    volume, residual = pl.pallas_call(
        kernel,
        out_shape=(jax.ShapeDtypeStruct((VP, FRAMES), F32), jax.ShapeDtypeStruct((RP, FRAMES), F32)),
        in_specs=[
            pl.BlockSpec(memory_space=pltpu.SMEM),
            pl.BlockSpec(memory_space=pl.ANY),
            pl.BlockSpec(memory_space=pltpu.VMEM),
        ],
        out_specs=(pl.BlockSpec(memory_space=pltpu.VMEM), pl.BlockSpec(memory_space=pltpu.VMEM)),
        scratch_shapes=[
            vm((TILE + 1, TILE, TILE), BF16),
            vm((NT, RAYS, TILE), BF16), vm((NT, VOX, TILE), BF16),
            vm((G, N_COL, M, RP), BF16), vm((G, N_ROW, M, VP), BF16),
            vm((G, nr, M, VP), BF16), vm((G, nr, M, VP), BF16),
            vm((G, nc, M, RP), BF16), vm((G, nc, M, RP), BF16),
            vm((G, M, VP), F32), vm((G, M, RP), F32),
            vm((G, M, VP), F32), vm((G, M, VP), F32), vm((G, M, RP), F32), vm((G, M, VP), F32), vm((G, M, RP), F32),
            vm((G, 1, 128), F32), vm((G, 1, 128), F32), vm((G, 1, 128), F32),
            vm((G, 1, 128), F32), vm((G, N_ROW, 1, 128), F32),
            vm((G, 1, 128), F32), vm((G, N_COL, 1, 128), F32), vm((G, 1, 128), F32), vm((G, N_COL, 1, 128), F32),
            dma, dma((G,)), dma((G,)), dma((G,)), dma((G,)), dma((G,)), dma((G,)),
            dma((G,)), dma((G,)), dma((G,)), dma((G,)), dma((G,)), dma((G,)), dma((G,)), dma((G,)),
        ],
        compiler_params=pltpu.CompilerParams(
            collective_id=0, has_side_effects=True, vmem_limit_bytes=60 * 1024 * 1024
        ),
    )(slot_of, tiles[0, 0], sinogram[0])
    return (volume[None], residual[None])


def solution(mesh):
    placed = (
        P("row", "col", None, None, None),
        P("row", "col", None),
        P("row", "col", None),
        P("row", "col"),
        P("row", "col", None),
    )
    return jax.shard_map(
        local,
        mesh=mesh,
        in_specs=placed,
        out_specs=(P("col", "row", None), P("row", "col", None)),
        check_vma=False,
    )
```

```python
import functools

import jax
import jax.numpy as jnp
from jax import lax
from jax.experimental import pallas as pl
from jax.experimental.pallas import tpu as pltpu
from jax.sharding import PartitionSpec as P

TILE = 128
NT = 16
ITERS = 4
NX = 4
N_ROW = 8
N_COL = 16
FRAMES = 128
RAYS = NT * TILE
VOX = NT * TILE
VP = VOX // N_ROW
RP = RAYS // N_COL
GROUPS = 2
M = FRAMES // GROUPS
MESH = pl.DeviceIdType.MESH
F32 = jnp.float32
BF16 = jnp.bfloat16

COL_PAIRS = (
    ((2, 2), (2, 1)),
    ((2, 3), (1, 2)),
    ((3, 2), (2, 0)),
    ((0, 2), (1, 1)),
    ((1, 3), (3, 1)),
    ((3, 3), (1, 0)),
    ((3, 0), (0, 1)),
    ((0, 3), (0, 0)),
)
COL_PEERS = tuple(d for pair in COL_PAIRS for d in pair)[:-1]
ROW_PEERS = tuple((dx, dc) for dx in (2, 1, 3, 0) for dc in (1, 0))[:-1]
BACK_BATCHES = (2, 3, 3)
BATCHES = (2, 3, 3)
FIRST = 0.6


def frame_squares(x):
    total = None
    for i in range(x.shape[1] // 128):
        part = x[:, i * 128 : (i + 1) * 128].astype(F32)
        total = part * part if total is None else total + part * part
    if M < 128:
        total = jnp.concatenate([total, jnp.zeros((128 - M, 128), F32)], axis=0)
    return jnp.sum(total.T, axis=0, keepdims=True)


def per_frame(*rows):
    stack = jnp.concatenate([*rows, jnp.zeros((8 - len(rows), 128), F32)], axis=0).T
    return [stack[:M, i : i + 1] for i in range(len(rows))]


def kernel(
    slots, tiles, sinogram, vol_out, res_out,
    slot_of, sino, tl, a, at, u, v, rsend, rrecv, csend, crecv, own_r, own_c,
    s, d, im, vol, res, gam, step, guess, nr_send, nr_recv, ng_send, ng_recv, ni_send, ni_recv,
    tsem, ssem, isem, u_ss, u_rs, v_ss, v_rs, r_ss, r_rs, c_ss, c_rs, nr_ss, nr_rs, ng_ss, ng_rs, ni_ss, ni_rs,
):
    row = lax.axis_index("row")
    col = lax.axis_index("col")
    x, core = row // 2, row % 2
    y, z = col // 4, col % 4

    def row_of(dx, dc):
        return ((x + dx) % 4) * 2 + (core + dc) % 2

    def col_of(dy, dz):
        return ((y + dy) % 4) * 4 + (z + dz) % 4

    def remote(src, dst, ss, rs, to_row, to_col):
        return pltpu.make_async_remote_copy(
            src_ref=src, dst_ref=dst, send_sem=ss, recv_sem=rs, device_id=(to_row, to_col), device_id_type=MESH
        )

    def arrived(ref, sem):
        remote(ref, ref, sem, sem, row, col).wait_recv()

    def sent(ref, sem):
        remote(ref, ref, sem, sem, row, col).wait_send()

    n_col, n_row = len(COL_PEERS), len(ROW_PEERS)

    def send_field(g):
        for dy, dz in COL_PEERS:
            remote(u.at[g, col], u.at[g, col], u_ss.at[g], u_rs.at[g], row, col_of(dy, dz)).start()

    def send_norm(g, i_send, i_recv, ss, rs):
        for i, (dy, dz) in enumerate(COL_PEERS):
            remote(i_send.at[g], i_recv.at[g, i], ss.at[g], rs.at[g], row, col_of(dy, dz)).start()

    def send_row_norm(g):
        for i, (dx, dc) in enumerate(ROW_PEERS):
            remote(nr_send.at[g], nr_recv.at[g, i], nr_ss.at[g], nr_rs.at[g], row_of(dx, dc), col).start()

    def r_send(g, i):
        return remote(rsend.at[g, i], rrecv.at[g, i], r_ss.at[g], r_rs.at[g], row_of(*ROW_PEERS[i]), col)

    def c_send(g, i):
        return remote(csend.at[g, i], crecv.at[g, i], c_ss.at[g], c_rs.at[g], row, col_of(*COL_PEERS[i]))

    def send_search(g):
        for dx, dc in ROW_PEERS:
            remote(v.at[g, row], v.at[g, row], v_ss.at[g], v_rs.at[g], row_of(dx, dc), col).start()

    def voxel_product(field, n):
        block = jnp.concatenate([a[2 * n], a[2 * n + 1]], axis=1)
        return jnp.dot(field, block, preferred_element_type=F32)

    def ray_product(field, first, second):
        block = jnp.concatenate([at[first], at[second]], axis=1)
        return jnp.dot(field, block, preferred_element_type=F32)

    def pass_norm(g):
        arrived(ni_recv.at[g, pl.ds(0, n_col)], ni_rs.at[g])
        squares = jnp.sum(ni_recv[g].reshape(N_COL, 128), axis=0, keepdims=True)
        nr_send[g] = squares
        nr_recv[g, n_row] = squares
        send_row_norm(g)
        sent(ni_recv.at[g, pl.ds(0, n_col)], ni_ss.at[g])

    def total_norm(g):
        arrived(nr_recv.at[g, pl.ds(0, n_row)], nr_rs.at[g])
        sent(nr_recv.at[g, pl.ds(0, n_row)], nr_ss.at[g])
        return jnp.sum(nr_recv[g].reshape(N_ROW, 128), axis=0, keepdims=True)

    def back_project(g):
        arrived(u.at[g, pl.ds(0, n_col)], u_rs.at[g])
        field = jnp.concatenate([u[g, i] for i in range(N_COL)], axis=1)
        done = 0
        for many in BACK_BATCHES:
            for i in range(done, done + many):
                if i < n_row:
                    rsend[g, i] = voxel_product(field, row_of(*ROW_PEERS[i])).astype(BF16)
                else:
                    own_r[g] = voxel_product(field, row)
            for i in range(done, min(done + many, n_row)):
                r_send(g, i).start()
            if done == 0:
                pass_norm(g)
            done += many
        sent(u.at[g, pl.ds(0, n_col)], u_ss.at[g])

    def new_search(g, k):
        norm = total_norm(g)
        new_step = jnp.where(k == 0, FIRST * norm, gam[g] / norm)
        alpha, share = per_frame(new_step, jnp.where(k == 0, 1.0, new_step / guess[g]))
        step[g] = new_step
        arrived(rrecv.at[g], r_rs.at[g])
        total = own_r[g]
        for i in range(n_row):
            total = total + rrecv[g, i].astype(F32)
        fresh = share * total + (1.0 - share) * s[g]
        s[g] = fresh
        v[g, row] = fresh.astype(BF16)
        send_search(g)
        vol[g] = vol[g] + alpha * d[g]
        res[g] = res[g] - alpha * im[g]
        sent(rsend.at[g], r_ss.at[g])

    def project(g):
        arrived(v.at[g, pl.ds(0, n_row)], v_rs.at[g])
        field = jnp.concatenate([v[g, i] for i in range(N_ROW)], axis=1)
        done = 0
        for many in BATCHES:
            for p in range(done, done + many):
                first, second = COL_PAIRS[p]
                part = ray_product(field, col_of(*first), col_of(*second))
                csend[g, 2 * p] = part[:, :RP].astype(BF16)
                if 2 * p + 1 < n_col:
                    csend[g, 2 * p + 1] = part[:, RP:].astype(BF16)
                else:
                    own_c[g] = part[:, RP:]
            if done == 0:
                squares = frame_squares(field)
                ng_send[g] = squares
                ng_recv[g, n_col] = squares
            for i in range(2 * done, min(2 * (done + many), n_col)):
                c_send(g, i).start()
            if done == 0:
                send_norm(g, ng_send, ng_recv, ng_ss, ng_rs)
            done += many
        sent(v.at[g, pl.ds(0, n_row)], v_ss.at[g])

    def new_image(g, k):
        arrived(ng_recv.at[g, pl.ds(0, n_col)], ng_rs.at[g])
        gamma = jnp.sum(ng_recv[g].reshape(N_COL, 128), axis=0, keepdims=True)
        ahead = jnp.where(k == 0, step[g] / gamma, step[g])
        ahead = jnp.where((ahead > 1e-30) & (ahead < 1e30), ahead, 1.0)
        beta, trial = per_frame(jnp.where(k == 0, 0.0, gamma / gam[g]), ahead)
        gam[g] = gamma
        guess[g] = ahead
        arrived(crecv.at[g], c_rs.at[g])
        total = own_c[g]
        for i in range(n_col):
            total = total + crecv[g, i].astype(F32)
        image = total + beta * im[g]
        im[g] = image

        @pl.when(k + 1 < ITERS)
        def _():
            u[g, col] = (res[g] - trial * image).astype(BF16)
            send_field(g)

        squares = frame_squares(image)
        ni_send[g] = squares
        ni_recv[g, n_col] = squares
        send_norm(g, ni_send, ni_recv, ni_ss, ni_rs)
        d[g] = s[g] + beta * d[g]
        sent(csend.at[g], c_ss.at[g])
        sent(ng_recv.at[g, pl.ds(0, n_col)], ng_ss.at[g])

    barrier = pltpu.get_barrier_semaphore()
    for dy, dz in COL_PEERS:
        pl.semaphore_signal(barrier, inc=1, device_id=(row, col_of(dy, dz)), device_id_type=MESH)
    for dx, dc in ROW_PEERS:
        pl.semaphore_signal(barrier, inc=1, device_id=(row_of(dx, dc), col), device_id_type=MESH)
    measure = pltpu.make_async_copy(sinogram, sino, ssem)
    measure.start()
    listed = pltpu.make_async_copy(slots, slot_of, isem)
    listed.start()
    load = pltpu.make_async_copy(tiles, tl.at[pl.ds(0, TILE)], tsem)
    load.start()
    measure.wait()
    first = sino[...].T
    for g in range(GROUPS):
        measured = first[g * M : (g + 1) * M]
        res[g] = measured
        u[g, col] = measured.astype(BF16)
        squares = frame_squares(measured)
        ni_send[g] = squares
        ni_recv[g, n_col] = squares
        s[g] = jnp.zeros((M, VP), F32)
        d[g] = jnp.zeros((M, VP), F32)
        vol[g] = jnp.zeros((M, VP), F32)
        im[g] = jnp.zeros((M, RP), F32)
        gam[g] = jnp.ones((1, 128), F32)
        guess[g] = jnp.ones((1, 128), F32)
    tl[TILE] = jnp.zeros((TILE, TILE), BF16)
    pl.semaphore_wait(barrier, n_col + n_row)
    for g in range(GROUPS):
        send_field(g)
        send_norm(g, ni_send, ni_recv, ni_ss, ni_rs)
    listed.wait()
    load.wait()

    def place(i, carry):
        for j in range(NT):
            rows = pl.ds(pl.multiple_of(i * TILE, TILE), TILE)
            a[j, rows, :] = tl[slot_of[i * NT + j]]
        return carry

    lax.fori_loop(0, NT, place, 0)

    def turn():
        places = [lax.broadcasted_iota(jnp.int32, (2 * TILE, 2 * TILE), i) for i in range(2)]
        one = jnp.where(places[0] == places[1], 1.0, 0.0).astype(BF16)

        def rows(i, carry):
            here = pl.ds(pl.multiple_of(i * 2 * TILE, 2 * TILE), 2 * TILE)
            for j in range(NT // 2):
                block = jnp.concatenate([a[2 * j, here, :], a[2 * j + 1, here, :]], axis=1)
                turned = lax.dot_general(one, block, (((1,), (1,)), ((), ())), preferred_element_type=F32).astype(BF16)
                at[2 * i, j * 2 * TILE : (j + 1) * 2 * TILE, :] = turned[:, :TILE]
                at[2 * i + 1, j * 2 * TILE : (j + 1) * 2 * TILE, :] = turned[:, TILE:]
            return carry

        lax.fori_loop(0, NT // 2, rows, 0)

    def iteration(k, carry):
        back_project(0)

        @pl.when(k == 0)
        def _():
            turn()

        if GROUPS == 1:
            new_search(0, k)
            project(0)
            new_image(0, k)
            return carry

        @pl.when(k > 0)
        def _():
            new_image(1, k - 1)

        new_search(0, k)
        back_project(1)
        project(0)
        new_search(1, k)
        new_image(0, k)
        project(1)
        return carry

    lax.fori_loop(0, ITERS, iteration, 0)

    def finish(g):
        (alpha,) = per_frame(gam[g] / total_norm(g))
        return vol[g] + alpha * d[g], res[g] - alpha * im[g]

    if GROUPS == 2:
        new_image(1, ITERS - 1)
    done = []
    for g in range(GROUPS):
        pass_norm(g)
    for g in range(GROUPS):
        done.append(finish(g))
    vol_out[...] = jnp.concatenate([volume for volume, _ in done], axis=0).T
    res_out[...] = jnp.concatenate([residual for _, residual in done], axis=0).T


def hand_over(vol_in, res_in, vol_out, res_out):
    vol_out[0] = vol_in[...]
    res_out[0] = res_in[...]


def local(tiles, tile_row, tile_col, tile_count, sinogram):
    live = jnp.arange(TILE, dtype=jnp.int32) < tile_count[0, 0]
    place = jnp.where(live, tile_row[0, 0] * NT + tile_col[0, 0], -1)
    slots = jnp.arange(TILE, dtype=jnp.int32)
    here = place[None, :] == jnp.arange(NT * NT, dtype=jnp.int32)[:, None]
    slot_of = jnp.min(jnp.where(here, slots[None, :], TILE), axis=1)
    dma = pltpu.SemaphoreType.DMA
    vm = pltpu.VMEM
    G, nc, nr = GROUPS, len(COL_PEERS), len(ROW_PEERS)
    volume, residual = pl.pallas_call(
        kernel,
        out_shape=(jax.ShapeDtypeStruct((VP, FRAMES), F32), jax.ShapeDtypeStruct((RP, FRAMES), F32)),
        in_specs=[
            pl.BlockSpec(memory_space=pl.ANY),
            pl.BlockSpec(memory_space=pl.ANY),
            pl.BlockSpec(memory_space=pl.ANY),
        ],
        out_specs=(pl.BlockSpec(memory_space=pltpu.VMEM), pl.BlockSpec(memory_space=pltpu.VMEM)),
        scratch_shapes=[
            pltpu.SMEM((NT * NT,), jnp.int32), vm((RP, FRAMES), F32),
            vm((TILE + 1, TILE, TILE), BF16),
            vm((NT, RAYS, TILE), BF16), vm((NT, VOX, TILE), BF16),
            vm((G, N_COL, M, RP), BF16), vm((G, N_ROW, M, VP), BF16),
            vm((G, nr, M, VP), BF16), vm((G, nr, M, VP), BF16),
            vm((G, nc, M, RP), BF16), vm((G, nc, M, RP), BF16),
            vm((G, M, VP), F32), vm((G, M, RP), F32),
            vm((G, M, VP), F32), vm((G, M, VP), F32), vm((G, M, RP), F32), vm((G, M, VP), F32), vm((G, M, RP), F32),
            vm((G, 1, 128), F32), vm((G, 1, 128), F32), vm((G, 1, 128), F32),
            vm((G, 1, 128), F32), vm((G, N_ROW, 1, 128), F32),
            vm((G, 1, 128), F32), vm((G, N_COL, 1, 128), F32), vm((G, 1, 128), F32), vm((G, N_COL, 1, 128), F32),
            dma, dma, dma, dma((G,)), dma((G,)), dma((G,)), dma((G,)), dma((G,)), dma((G,)),
            dma((G,)), dma((G,)), dma((G,)), dma((G,)), dma((G,)), dma((G,)), dma((G,)), dma((G,)),
        ],
        compiler_params=pltpu.CompilerParams(
            collective_id=0, has_side_effects=True, vmem_limit_bytes=60 * 1024 * 1024
        ),
    )(slot_of, tiles[0, 0], sinogram[0])
    return pl.pallas_call(
        hand_over,
        out_shape=(jax.ShapeDtypeStruct((1, VP, FRAMES), F32), jax.ShapeDtypeStruct((1, RP, FRAMES), F32)),
    )(volume, residual)


def solution(mesh):
    placed = (
        P("row", "col", None, None, None),
        P("row", "col", None),
        P("row", "col", None),
        P("row", "col"),
        P("row", "col", None),
    )
    return jax.shard_map(
        local,
        mesh=mesh,
        in_specs=placed,
        out_specs=(P("col", "row", None), P("row", "col", None)),
        check_vma=False,
    )
```
